8 devices in a mesh: dp: 2 (over z, y), sp: 4 (over x, core).
Axes of the slice: x: 2, y: 2, z: 1, core: 2. Of those that a mesh axis runs over, the one named last changes fastest.
Arguments:
- hidden: bfloat16 [32, 1024, 2560], P('dp', 'sp'), parts along dimension 0
- seq_lens: int32 [32], P('dp'), parts along dimension 0
- ln1_gain: float32 [2560], replicated
- ln1_bias: float32 [2560], replicated
- ln2_gain: float32 [2560], replicated
- ln2_bias: float32 [2560], replicated
- w_qkv: bfloat16 [2560, 7680], replicated
- b_qkv: float32 [32, 3, 80], replicated
- w_out: bfloat16 [2560, 2560], replicated
- b_out: float32 [2560], replicated
- w_up: bfloat16 [2560, 10240], replicated
- b_up: float32 [10240], replicated
- w_down: bfloat16 [10240, 2560], replicated
- b_down: float32 [2560], replicated
Outputs:
- output 1: bfloat16 [32, 1024, 2560], P('dp', 'sp'), parts along dimension 0
- output 2: bfloat16 [32, 32, 1024, 80], P('dp', 'sp'), parts along dimension 0
- output 3: bfloat16 [32, 32, 1024, 80], P('dp', 'sp'), parts along dimension 0
There are 2 independent parts. The reference program is written for one: setup_inputs(seed, part) draws one part's arguments, and reference() takes and returns one part's arrays. A program takes and returns all parts, laid end to end along the dimension named above; an argument that names none is the same for every part.
All inputs are finite; a program needn't handle non-finite values.
Results may differ from the reference program's by a relative error of at most 0.00451203.
Values are sent between devices in bfloat16 or wider.
A program may use at most 1 GiB of HBM per device.

```python
import jax
import jax.numpy as jnp
from jax import lax

BATCH_SEQS = 16
SEQ_SHARDS = 4
ROWS_DEV = 256
D_MODEL = 2560
N_HEADS = 32
HEAD_DIM = 80
D_FF = 10240

SEQ_LEN = ROWS_DEV * SEQ_SHARDS
ROT_DIM = HEAD_DIM // 4
LN_EPS = 1e-5
ROT_BASE = 10000.0


def setup_inputs(seed: int = 0, part: int = 0) -> dict:
    part_key = jax.random.fold_in(jax.random.key(seed), part)
    shared = jax.random.split(jax.random.key(seed + 7919), 12)
    key_x, key_len, key_full = jax.random.split(part_key, 3)
    hidden = jax.random.normal(key_x, (BATCH_SEQS, SEQ_LEN, D_MODEL), jnp.float32).astype(jnp.bfloat16)
    drawn = jax.random.randint(key_len, (BATCH_SEQS,), SEQ_LEN // 2 + 1, SEQ_LEN + 1, jnp.int32)
    full_row = jax.random.randint(key_full, (), 0, BATCH_SEQS, jnp.int32)
    seq_lens = jnp.where(jnp.arange(BATCH_SEQS) == full_row, SEQ_LEN, drawn).astype(jnp.int32)

    def gauss(key, shape, scale):
        return jax.random.normal(key, shape, jnp.float32) * scale

    return {
        'hidden': hidden,
        'seq_lens': seq_lens,
        'ln1_gain': 1.0 + gauss(shared[0], (D_MODEL,), 0.2),
        'ln1_bias': gauss(shared[1], (D_MODEL,), 0.2),
        'ln2_gain': 1.0 + gauss(shared[2], (D_MODEL,), 0.2),
        'ln2_bias': gauss(shared[3], (D_MODEL,), 0.2),
        'w_qkv': gauss(shared[4], (D_MODEL, 3 * D_MODEL), 1.5 * D_MODEL ** -0.5).astype(jnp.bfloat16),
        'b_qkv': gauss(shared[5], (N_HEADS, 3, HEAD_DIM), 0.3),
        'w_out': gauss(shared[6], (D_MODEL, D_MODEL), D_MODEL ** -0.5).astype(jnp.bfloat16),
        'b_out': gauss(shared[7], (D_MODEL,), 0.3),
        'w_up': gauss(shared[8], (D_MODEL, D_FF), D_MODEL ** -0.5).astype(jnp.bfloat16),
        'b_up': gauss(shared[9], (D_FF,), 0.3),
        'w_down': gauss(shared[10], (D_FF, D_MODEL), 1.5 * D_FF ** -0.5).astype(jnp.bfloat16),
        'b_down': gauss(shared[11], (D_MODEL,), 0.3),
    }


def layer_norm(rows, gain, shift):
    rows32 = rows.astype(jnp.float32)
    centered = rows32 - jnp.mean(rows32, axis=-1, keepdims=True)
    variance = jnp.mean(centered * centered, axis=-1, keepdims=True)
    return (centered * lax.rsqrt(variance + LN_EPS) * gain + shift).astype(jnp.bfloat16)


def rotary(vecs, positions):
    half_rot = ROT_DIM // 2
    inv_freq = ROT_BASE ** (-2.0 * jnp.arange(half_rot, dtype=jnp.float32) / ROT_DIM)
    angles = positions.astype(jnp.float32)[:, None] * inv_freq[None, :]
    cosines = jnp.cos(angles)[:, None, :]
    sines = jnp.sin(angles)[:, None, :]
    first = vecs[..., :half_rot]
    second = vecs[..., half_rot:ROT_DIM]
    return jnp.concatenate([first * cosines - second * sines, second * cosines + first * sines, vecs[..., ROT_DIM:]], axis=-1)


def reference(hidden, seq_lens, ln1_gain, ln1_bias, ln2_gain, ln2_bias, w_qkv, b_qkv, w_out, b_out, w_up, b_up, w_down, b_down):
    n_blocks = BATCH_SEQS * SEQ_SHARDS
    row_blocks = hidden.reshape(n_blocks, ROWS_DEV, D_MODEL)
    block_start = (jnp.arange(n_blocks) % SEQ_SHARDS) * ROWS_DEV

    def project(operands):
        rows, start = operands
        normed = layer_norm(rows, ln1_gain, ln1_bias)
        proj_qkv = jnp.dot(normed, w_qkv, preferred_element_type=jnp.float32)
        proj_qkv = proj_qkv.reshape(ROWS_DEV, N_HEADS, 3, HEAD_DIM) + b_qkv
        positions = start + jnp.arange(ROWS_DEV)
        q_rows = rotary(proj_qkv[:, :, 0], positions).astype(jnp.bfloat16)
        k_rows = rotary(proj_qkv[:, :, 1], positions).astype(jnp.bfloat16)
        v_rows = proj_qkv[:, :, 2].astype(jnp.bfloat16)
        return q_rows, k_rows, v_rows

    q_all, k_all, v_all = lax.map(project, (row_blocks, block_start))
    q_heads = jnp.transpose(q_all.reshape(BATCH_SEQS, SEQ_LEN, N_HEADS, HEAD_DIM), (2, 0, 1, 3))
    k_cache = jnp.transpose(k_all.reshape(BATCH_SEQS, SEQ_LEN, N_HEADS, HEAD_DIM), (0, 2, 1, 3))
    v_cache = jnp.transpose(v_all.reshape(BATCH_SEQS, SEQ_LEN, N_HEADS, HEAD_DIM), (0, 2, 1, 3))
    key_pos = jnp.arange(SEQ_LEN)
    score_scale = HEAD_DIM ** -0.5

    def one_head(operands):
        q_one, k_one, v_one = operands
        k_wide = k_one.astype(jnp.float32)
        v_wide = v_one.astype(jnp.float32)

        def one_block(start):
            q_blk = lax.dynamic_slice_in_dim(q_one, start, ROWS_DEV, axis=1).astype(jnp.float32)
            scores = jnp.einsum('bqd,bkd->bqk', q_blk, k_wide) * score_scale
            q_pos = start + jnp.arange(ROWS_DEV)
            allowed = (key_pos[None, None, :] <= q_pos[None, :, None]) & (key_pos[None, None, :] < seq_lens[:, None, None])
            scores = jnp.where(allowed, scores, -jnp.inf)
            weights = jnp.exp(scores - jnp.max(scores, axis=-1, keepdims=True))
            total = jnp.sum(weights, axis=-1, keepdims=True)
            rounded = weights.astype(jnp.bfloat16).astype(jnp.float32)
            context = jnp.einsum('bqk,bkd->bqd', rounded, v_wide) / total
            return context.astype(jnp.bfloat16)

        blocks = lax.map(one_block, jnp.arange(SEQ_SHARDS) * ROWS_DEV)
        return jnp.transpose(blocks, (1, 0, 2, 3)).reshape(BATCH_SEQS, SEQ_LEN, HEAD_DIM)

    k_for_heads = jnp.transpose(k_cache, (1, 0, 2, 3))
    v_for_heads = jnp.transpose(v_cache, (1, 0, 2, 3))
    context = lax.map(one_head, (q_heads, k_for_heads, v_for_heads))
    ctx_blocks = jnp.transpose(context, (1, 2, 0, 3)).reshape(n_blocks, ROWS_DEV, D_MODEL)

    def finish(operands):
        rows, ctx_rows = operands
        attn_out = jnp.dot(ctx_rows, w_out, preferred_element_type=jnp.float32) + b_out
        normed = layer_norm(rows, ln2_gain, ln2_bias)
        pre_act = jnp.dot(normed, w_up, preferred_element_type=jnp.float32) + b_up
        hidden_act = jax.nn.gelu(pre_act, approximate=False).astype(jnp.bfloat16)
        mlp_out = jnp.dot(hidden_act, w_down, preferred_element_type=jnp.float32) + b_down
        return (rows.astype(jnp.float32) + attn_out + mlp_out).astype(jnp.bfloat16)

    out_blocks = lax.map(finish, (row_blocks, ctx_blocks))
    return out_blocks.reshape(BATCH_SEQS, SEQ_LEN, D_MODEL), k_cache, v_cache
```

```python
import functools

import jax
import jax.numpy as jnp
from jax import lax
from jax.experimental import pallas as pl
from jax.experimental.pallas import tpu as pltpu
from jax.sharding import PartitionSpec as P

LN_EPS = 1e-5
ROT_BASE = 10000.0
LOG2_E = 1.4426950408889634


def rotary_tables(n_positions, head_dim):
    rot_dim = head_dim // 4
    half_rot = rot_dim // 2
    inv_freq = ROT_BASE ** (-2.0 * jnp.arange(half_rot, dtype=jnp.float32) / rot_dim)
    angles = inv_freq[:, None] * jnp.arange(n_positions).astype(jnp.float32)[None, :]
    cosines, sines = jnp.cos(angles), jnp.sin(angles)
    rest = jnp.zeros((-rot_dim % 8, n_positions), jnp.float32)
    zeros = jnp.zeros_like(sines)
    keep = jnp.concatenate([cosines, cosines, rest + 1.0], axis=0)
    below = jnp.concatenate([-sines, zeros, rest], axis=0)
    above = jnp.concatenate([zeros, sines, rest], axis=0)
    return keep, below, above


def norm_kernel(x_ref, g1_ref, b1_ref, g2_ref, b2_ref, a_ref, m_ref):
    rows = x_ref[0].astype(jnp.float32)
    centered = rows - jnp.mean(rows, axis=-1, keepdims=True)
    variance = jnp.mean(centered * centered, axis=-1, keepdims=True)
    normed = centered * lax.rsqrt(variance + LN_EPS)
    a_ref[0] = (normed * g1_ref[...] + b1_ref[...]).astype(jnp.bfloat16)
    m_ref[0] = (normed * g2_ref[...] + b2_ref[...]).astype(jnp.bfloat16)


def norms(hidden, first, count, g1, b1, g2, b2):
    _, rows, width = hidden.shape
    block = pl.BlockSpec((1, rows, width), lambda i: (i, 0, 0))
    vec = pl.BlockSpec((1, width), lambda i: (0, 0))
    shape = jax.ShapeDtypeStruct((count, rows, width), jnp.bfloat16)
    return pl.pallas_call(
        norm_kernel,
        grid=(count,),
        in_specs=[pl.BlockSpec((1, rows, width), lambda i: (i + first, 0, 0)), vec, vec, vec, vec],
        out_specs=[block, block],
        out_shape=[shape, shape],
        cost_estimate=pl.CostEstimate(flops=count * rows * width * 200, bytes_accessed=count * rows * width * 6, transcendentals=0),
        name="norms",
    )(hidden, g1, b1, g2, b2)


def turn_kernel(shard_ref, w_ref, out_ref):
    out_ref[...] = w_ref[...].T


def turned_columns(w, shard, n_shards):
    depth, columns = w.shape
    span, piece = columns // n_shards, 256
    return pl.pallas_call(
        turn_kernel,
        grid_spec=pltpu.PrefetchScalarGridSpec(
            num_scalar_prefetch=1,
            grid=(depth // piece,),
            in_specs=[pl.BlockSpec((piece, span), lambda i, shard: (i, shard[0]))],
            out_specs=pl.BlockSpec((span, piece), lambda i, shard: (0, i)),
        ),
        out_shape=jax.ShapeDtypeStruct((span, depth), w.dtype),
        cost_estimate=pl.CostEstimate(flops=depth * span * 1000, bytes_accessed=depth * span * 4, transcendentals=0),
        name="turn",
    )(shard, w)


def attn_kernel(count, n_heads, head_dim, rows, prev, info_ref, len_ref, a0, a1, a2, a3, w_ref, bias_ref, keep_ref, below_ref, above_ref, *rest):
    k_out, v_out, c0, c1, c2, c3, qkv_a, qkv_b, k_turned, ctx_buf = rest[prev:]
    step = pl.program_id(0)
    me = info_ref[0]
    sources = (a0, a1, a2, a3)
    n_blocks = len(sources)
    scale = LOG2_E * head_dim ** -0.5
    half_rot = head_dim // 8
    turning = keep_ref.shape[0]
    span = 3 * head_dim

    length = len_ref[step + info_ref[1]]
    key = lax.broadcasted_iota(jnp.int32, (rows, rows), 0)
    causal = key <= lax.broadcasted_iota(jnp.int32, (rows, rows), 1)

    def project(head, j, qkv):
        at = pl.ds(pl.multiple_of((me ^ j) * rows, rows), rows)
        w_rows = w_ref[pl.ds(pl.multiple_of(head * span, span), span)]
        out = lax.dot_general(w_rows, sources[j][0], (((1,), (1,)), ((), ())), preferred_element_type=jnp.float32) + bias_ref[head]
        keep, below, above = keep_ref[:, at], below_ref[:, at], above_ref[:, at]

        def rotate(u):
            first = u[:turning]
            first = first * keep + pltpu.roll(first, turning - half_rot, 0) * below + pltpu.roll(first, half_rot, 0) * above
            return jnp.concatenate([first, u[turning:]], axis=0).astype(jnp.bfloat16)

        k_cols = rotate(out[head_dim:2 * head_dim])
        v_cols = out[2 * head_dim:].astype(jnp.bfloat16)
        qkv[:head_dim, at] = rotate(out[:head_dim])
        qkv[head_dim:2 * head_dim, at] = k_cols
        qkv[2 * head_dim:, at] = v_cols
        k_out[0, head, :, at] = k_cols
        v_out[0, head, :, at] = v_cols

    def turn(qkv):
        k_turned[...] = qkv[head_dim:2 * head_dim].T

    def score(block, qkv):
        q_cols = qkv[:head_dim, pl.ds(block * rows, rows)]
        parts = []
        for j in range(block + 1):
            s = jnp.dot(k_turned[pl.ds(j * rows, rows)], q_cols, preferred_element_type=jnp.float32)
            if j == block:
                s = jnp.where(causal, s, -jnp.inf)
            if (j + 1) * rows > n_blocks * rows // 2:
                s = jnp.where(key < length - j * rows, s, -jnp.inf)
            parts.append(s)
        return parts

    def mix(head, block, qkv, parts):
        at = pl.ds(block * rows, rows)
        top = functools.reduce(jnp.maximum, parts)
        top = jnp.max(top, axis=0, keepdims=True)
        parts = [jnp.exp2((s - top) * scale) for s in parts]
        total = jnp.sum(functools.reduce(jnp.add, parts), axis=0, keepdims=True)
        weights = jnp.concatenate([p.astype(jnp.bfloat16) for p in parts], axis=0)
        context = jnp.dot(qkv[2 * head_dim:, pl.ds(0, (block + 1) * rows)], weights, preferred_element_type=jnp.float32)
        ctx_buf[pl.ds(pl.multiple_of(head * head_dim, head_dim), head_dim), at] = (context / total).astype(jnp.bfloat16)

    def head_step(head, qkv, next_head, next_qkv):
        turn(qkv)
        parts = score(0, qkv)
        for block in range(n_blocks):
            after = score(block + 1, qkv) if block + 1 < n_blocks else None
            project(next_head, block, next_qkv)
            mix(head, block, qkv, parts)
            parts = after

    for j in range(n_blocks):
        project(0, j, qkv_a)

    def pair(t, carry):
        head_step(2 * t, qkv_a, 2 * t + 1, qkv_b)
        head_step(2 * t + 1, qkv_b, 2 * t + 2, qkv_a)
        return carry

    lax.fori_loop(0, n_heads // 2 - 1, pair, 0)
    head_step(n_heads - 2, qkv_a, n_heads - 1, qkv_b)
    turn(qkv_b)
    parts = score(0, qkv_b)
    for block in range(n_blocks):
        after = score(block + 1, qkv_b) if block + 1 < n_blocks else None
        mix(n_heads - 1, block, qkv_b, parts)
        parts = after

    for j, out in enumerate((c0, c1, c2, c3)):
        out[0] = ctx_buf[:, pl.ds(pl.multiple_of((me ^ j) * rows, rows), rows)].T


def whole(shape):
    return pl.BlockSpec(shape, lambda i, *_: (0,) * len(shape), pipeline_mode=pl.Buffered(1))


def attention(info, lens, sources, w_turned, bias, tables, caches, n_prompts, first):
    count, rows, width = sources[0].shape
    n_heads, span, _ = bias.shape
    head_dim = span // 3
    seq = rows * len(sources)
    prev = 0 if caches is None else 2
    hbm = pl.BlockSpec(memory_space=pl.ANY)
    source_spec = pl.BlockSpec((1, rows, width), lambda i, *_: (i, 0, 0))
    table = whole(tables[0].shape)
    cache_shape = jax.ShapeDtypeStruct((n_prompts, n_heads, head_dim, seq), jnp.bfloat16)
    cache_spec = pl.BlockSpec((1, n_heads, head_dim, seq), lambda i, *_: (i + first, 0, 0, 0))
    ctx_shape = jax.ShapeDtypeStruct((count, rows, n_heads * head_dim), jnp.bfloat16)
    ctx_spec = pl.BlockSpec((1, rows, n_heads * head_dim), lambda i, *_: (i, 0, 0))
    columns = pltpu.VMEM((span, seq), jnp.bfloat16)
    flops = count * seq * width * n_heads * 256 * 2 + count * n_heads * seq * seq * 256 * 2
    return pl.pallas_call(
        functools.partial(attn_kernel, count, n_heads, head_dim, rows, prev),
        grid_spec=pltpu.PrefetchScalarGridSpec(
            num_scalar_prefetch=2,
            grid=(count,),
            in_specs=[source_spec] * 4 + [whole(w_turned.shape), whole(bias.shape), table, table, table] + [hbm] * prev,
            out_specs=[cache_spec, cache_spec] + [ctx_spec] * 4,
            scratch_shapes=[columns, columns, pltpu.VMEM((seq, head_dim), jnp.bfloat16), pltpu.VMEM((n_heads * head_dim, seq), jnp.bfloat16)],
        ),
        out_shape=[cache_shape, cache_shape] + [ctx_shape] * 4,
        input_output_aliases={11: 0, 12: 1} if prev else {},
        compiler_params=pltpu.CompilerParams(dimension_semantics=("arbitrary",), vmem_limit_bytes=58 * 1024 * 1024),
        cost_estimate=pl.CostEstimate(flops=flops, bytes_accessed=count * seq * width * 4, transcendentals=count * n_heads * seq * seq // 2),
        name="qkv_attention",
    )(info, lens, *sources, w_turned, bias, *tables, *(caches or ()))


def out_kernel(n_groups, n_shards, count, shard_ref, x_ref, b_out_ref, b_down_ref, *rest):
    mlps, rest = rest[:n_groups], rest[n_groups:]
    contexts, rest = rest[:n_groups * n_shards], rest[n_groups * n_shards:]
    weights, out_ref = rest[:n_shards], rest[-1]
    for g in range(n_groups):
        @pl.when(pl.program_id(0) // count == g)
        def _(g=g):
            attn = b_out_ref[...]
            for c_ref, w_ref in zip(contexts[g * n_shards:(g + 1) * n_shards], weights):
                attn = attn + jnp.dot(c_ref[0], w_ref[...], preferred_element_type=jnp.float32)
            out_ref[0] = (x_ref[0].astype(jnp.float32) + attn + (mlps[g][0] + b_down_ref[...])).astype(jnp.bfloat16)


def finish(shard, hidden, mlps, b_out, b_down, contexts, w_out, prev, first):
    n_groups, n_shards = len(contexts), len(contexts[0])
    count, rows, span = contexts[0][0].shape
    width = hidden.shape[-1]
    far = pl.BlockSpec((1, rows, width), lambda i, *_: (i + first, 0, 0))

    def near(columns, g):
        return pl.BlockSpec((1, rows, columns), lambda i, *_: (jnp.clip(i - g * count, 0, count - 1), 0, 0))

    w_specs = [
        pl.BlockSpec((span, width), lambda i, shard, j=j: (shard[0] ^ j, 0), pipeline_mode=pl.Buffered(1)) for j in range(n_shards)
    ]
    aliased = [] if prev is None else [prev]
    in_specs = [far, whole((1, width)), whole((1, width))] + [near(width, g) for g in range(n_groups)]
    in_specs += [near(span, g) for g in range(n_groups) for _ in range(n_shards)] + w_specs
    operands = [shard, hidden, b_out, b_down, *mlps, *(c for group in contexts for c in group), *([w_out] * n_shards)]
    total = n_groups * count
    return pl.pallas_call(
        functools.partial(out_kernel, n_groups, n_shards, count),
        grid_spec=pltpu.PrefetchScalarGridSpec(
            num_scalar_prefetch=1,
            grid=(total,),
            in_specs=in_specs + [pl.BlockSpec(memory_space=pl.ANY)] * len(aliased),
            out_specs=far,
        ),
        out_shape=jax.ShapeDtypeStruct(hidden.shape, jnp.bfloat16),
        input_output_aliases={len(operands): 0} if aliased else {},
        compiler_params=pltpu.CompilerParams(dimension_semantics=("arbitrary",), vmem_limit_bytes=58 * 1024 * 1024),
        cost_estimate=pl.CostEstimate(flops=total * rows * width * width * 2, bytes_accessed=total * rows * width * 10, transcendentals=0),
        name="finish",
    )(*operands, *aliased)


def solution(mesh):
    n_shards = mesh.shape['sp']
    row_spec = P('dp', 'sp', None)
    cache_spec = P('dp', 'sp', None, None)
    vec_spec = P(None)
    mat_spec = P(None, None)
    n_groups = 4

    def swap(array, mask):
        return lax.ppermute(array, 'sp', [(i, i ^ mask) for i in range(n_shards)])

    def local_layer(hidden, seq_lens, ln1_gain, ln1_bias, ln2_gain, ln2_bias, w_qkv, b_qkv, w_out, b_out, w_up, b_up, w_down, b_down):
        n_prompts, rows, width = hidden.shape
        n_heads, _, head_dim = b_qkv.shape
        own_heads = n_heads // n_shards
        shard = lax.axis_index('sp')
        count = n_prompts // n_groups

        normed = [norms(hidden, g * count, count, ln1_gain[None], ln1_bias[None], ln2_gain[None], ln2_bias[None]) for g in range(n_groups)]
        gathered = []
        for attn_in, _ in normed:
            far = swap(attn_in, 2)
            gathered.append((attn_in, swap(attn_in, 1), far, swap(far, 1)))

        where = shard.astype(jnp.int32).reshape(1)
        w_turned = turned_columns(w_qkv, where, n_shards)
        b_heads = lax.dynamic_slice_in_dim(b_qkv, shard * own_heads, own_heads, axis=0).reshape(own_heads, 3 * head_dim, 1)
        tables = rotary_tables(rows * n_shards, head_dim)

        def up(g):
            pre = jnp.dot(normed[g][1].reshape(count * rows, width), w_up, preferred_element_type=jnp.float32) + b_up
            return (0.5 * pre * (1.0 + lax.erf(pre * (0.5 ** 0.5)))).astype(jnp.bfloat16)

        acts = [up(g) for g in range(n_groups)]
        caches = None
        contexts = []
        for g in range(n_groups):
            info = jnp.stack([shard, jnp.int32(g * count)]).astype(jnp.int32)
            k_cache, v_cache, *ctx = attention(info, seq_lens, gathered[g], w_turned, b_heads, tables, caches, n_prompts, g * count)
            caches = (k_cache, v_cache)
            contexts.append([ctx[0]] + [swap(ctx[j], j) for j in range(1, n_shards)])
        mlps = [jnp.dot(act, w_down, preferred_element_type=jnp.float32).reshape(count, rows, width) for act in acts]
        split = n_groups - 1
        out = finish(where, hidden, mlps[:split], b_out[None], b_down[None], contexts[:split], w_out, None, 0)
        out = finish(where, hidden, mlps[split:], b_out[None], b_down[None], contexts[split:], w_out, out, split * count)
        return out, jnp.swapaxes(caches[0], 2, 3), jnp.swapaxes(caches[1], 2, 3)

    return jax.shard_map(local_layer, mesh=mesh,
                         in_specs=(row_spec, P('dp'), vec_spec, vec_spec, vec_spec, vec_spec, mat_spec, P(None, None, None), mat_spec, vec_spec, mat_spec, vec_spec, mat_spec, vec_spec),
                         out_specs=(row_spec, cache_spec, cache_spec), check_vma=False)
```

```python
import functools

import jax
import jax.numpy as jnp
from jax import lax
from jax.experimental import pallas as pl
from jax.experimental.pallas import tpu as pltpu
from jax.sharding import PartitionSpec as P


LN_EPS = 1e-5
ROT_BASE = 10000.0
LOG2_E = 1.4426950408889634


def rotary_tables(n_positions, head_dim):
    rot_dim = head_dim // 4
    half_rot = rot_dim // 2
    inv_freq = ROT_BASE ** (-2.0 * jnp.arange(half_rot, dtype=jnp.float32) / rot_dim)
    angles = inv_freq[:, None] * jnp.arange(n_positions).astype(jnp.float32)[None, :]
    cosines, sines = jnp.cos(angles), jnp.sin(angles)
    rest = jnp.zeros((-rot_dim % 8, n_positions), jnp.float32)
    zeros = jnp.zeros_like(sines)
    keep = jnp.concatenate([cosines, cosines, rest + 1.0], axis=0)
    below = jnp.concatenate([-sines, zeros, rest], axis=0)
    above = jnp.concatenate([zeros, sines, rest], axis=0)
    return keep, below, above


def norm_kernel(n_halves, n_prompts, x_ref, g1_ref, b1_ref, g2_ref, b2_ref, *outs):
    step = pl.program_id(0)
    rows = x_ref[0].astype(jnp.float32)
    centered = rows - jnp.mean(rows, axis=-1, keepdims=True)
    variance = jnp.mean(centered * centered, axis=-1, keepdims=True)
    normed = centered * lax.rsqrt(variance + LN_EPS)
    a_rows = (normed * g1_ref[...] + b1_ref[...]).astype(jnp.bfloat16)
    m_rows = (normed * g2_ref[...] + b2_ref[...]).astype(jnp.bfloat16)
    for parts, result in ((outs[:n_halves], a_rows), (outs[n_halves:], m_rows)):
        size = n_prompts // len(parts)
        for g, part in enumerate(parts):
            @pl.when(step // size == g)
            def _(part=part, result=result):
                part[0] = result


def part_spec(shape, start, count):
    return pl.BlockSpec((1,) + shape, lambda i, *_: (jnp.clip(i - start, 0, count - 1), 0, 0))


def norms(hidden, n_halves, n_quarters, g1, b1, g2, b2):
    n_prompts, rows, width = hidden.shape
    vec = pl.BlockSpec((1, width), lambda i: (0, 0))
    parts = [(g * (n_prompts // n), n_prompts // n) for n in (n_halves, n_quarters) for g in range(n)]
    return pl.pallas_call(
        functools.partial(norm_kernel, n_halves, n_prompts),
        grid=(n_prompts,),
        in_specs=[pl.BlockSpec((1, rows, width), lambda i: (i, 0, 0)), vec, vec, vec, vec],
        out_specs=[part_spec((rows, width), *part) for part in parts],
        out_shape=[jax.ShapeDtypeStruct((count, rows, width), jnp.bfloat16) for _, count in parts],
        compiler_params=pltpu.CompilerParams(dimension_semantics=("arbitrary",)),
        cost_estimate=pl.CostEstimate(flops=n_prompts * rows * width * 200, bytes_accessed=n_prompts * rows * width * 6, transcendentals=0),
        name="norms",
    )(hidden, g1, b1, g2, b2)


def turn_kernel(shard_ref, w_ref, out_ref):
    out_ref[...] = w_ref[...].T


def turned_columns(w, shard, n_shards):
    depth, columns = w.shape
    span, piece = columns // n_shards, 256
    return pl.pallas_call(
        turn_kernel,
        grid_spec=pltpu.PrefetchScalarGridSpec(
            num_scalar_prefetch=1,
            grid=(depth // piece,),
            in_specs=[pl.BlockSpec((piece, span), lambda i, shard: (i, shard[0]))],
            out_specs=pl.BlockSpec((span, piece), lambda i, shard: (0, i)),
        ),
        out_shape=jax.ShapeDtypeStruct((span, depth), w.dtype),
        cost_estimate=pl.CostEstimate(flops=depth * span * 1000, bytes_accessed=depth * span * 4, transcendentals=0),
        name="turn",
    )(shard, w)


def attn_kernel(n_heads, head_dim, rows, prev, info_ref, len_ref, a0, a1, a2, a3, w_ref, bias_ref, keep_ref, below_ref, above_ref, *rest):
    k_out, v_out, c0, c1, c2, c3, qkv_a, qkv_b, k_turned, ctx_buf = rest[prev:]
    step = pl.program_id(0)
    me = info_ref[0]
    sources = (a0, a1, a2, a3)
    n_blocks = len(sources)
    scale = LOG2_E * head_dim ** -0.5
    half_rot = head_dim // 8
    turning = keep_ref.shape[0]
    span = 3 * head_dim

    length = len_ref[step + info_ref[1]]
    key = lax.broadcasted_iota(jnp.int32, (rows, rows), 0)
    causal = key <= lax.broadcasted_iota(jnp.int32, (rows, rows), 1)

    def project(head, j, qkv):
        at = pl.ds(pl.multiple_of((me ^ j) * rows, rows), rows)
        w_rows = w_ref[pl.ds(pl.multiple_of(head * span, span), span)]
        out = lax.dot_general(w_rows, sources[j][0], (((1,), (1,)), ((), ())), preferred_element_type=jnp.float32) + bias_ref[head]
        keep, below, above = keep_ref[:, at], below_ref[:, at], above_ref[:, at]

        def rotate(u):
            first = u[:turning]
            first = first * keep + pltpu.roll(first, turning - half_rot, 0) * below + pltpu.roll(first, half_rot, 0) * above
            return jnp.concatenate([first, u[turning:]], axis=0).astype(jnp.bfloat16)

        k_cols = rotate(out[head_dim:2 * head_dim])
        v_cols = out[2 * head_dim:].astype(jnp.bfloat16)
        qkv[:head_dim, at] = rotate(out[:head_dim])
        qkv[head_dim:2 * head_dim, at] = k_cols
        qkv[2 * head_dim:, at] = v_cols
        k_out[0, head, :, at] = k_cols
        v_out[0, head, :, at] = v_cols

    def turn(qkv):
        k_turned[...] = qkv[head_dim:2 * head_dim].T

    def score(block, qkv):
        q_cols = qkv[:head_dim, pl.ds(block * rows, rows)]
        parts = []
        for j in range(block + 1):
            s = jnp.dot(k_turned[pl.ds(j * rows, rows)], q_cols, preferred_element_type=jnp.float32)
            if j == block:
                s = jnp.where(causal, s, -jnp.inf)
            if (j + 1) * rows > n_blocks * rows // 2:
                s = jnp.where(key < length - j * rows, s, -jnp.inf)
            parts.append(s)
        return parts

    def mix(head, block, qkv, parts):
        at = pl.ds(block * rows, rows)
        top = functools.reduce(jnp.maximum, parts)
        top = jnp.max(top, axis=0, keepdims=True)
        parts = [jnp.exp2((s - top) * scale) for s in parts]
        total = jnp.sum(functools.reduce(jnp.add, parts), axis=0, keepdims=True)
        weights = jnp.concatenate([p.astype(jnp.bfloat16) for p in parts], axis=0)
        context = jnp.dot(qkv[2 * head_dim:, pl.ds(0, (block + 1) * rows)], weights, preferred_element_type=jnp.float32)
        ctx_buf[pl.ds(pl.multiple_of(head * head_dim, head_dim), head_dim), at] = (context / total).astype(jnp.bfloat16)

    def head_step(head, qkv, next_head, next_qkv):
        turn(qkv)
        parts = score(0, qkv)
        for block in range(n_blocks):
            after = score(block + 1, qkv) if block + 1 < n_blocks else None
            project(next_head, block, next_qkv)
            mix(head, block, qkv, parts)
            parts = after

    for j in range(n_blocks):
        project(0, j, qkv_a)

    def pair(t, carry):
        head_step(2 * t, qkv_a, 2 * t + 1, qkv_b)
        head_step(2 * t + 1, qkv_b, 2 * t + 2, qkv_a)
        return carry

    lax.fori_loop(0, n_heads // 2 - 1, pair, 0)
    head_step(n_heads - 2, qkv_a, n_heads - 1, qkv_b)
    turn(qkv_b)
    parts = score(0, qkv_b)
    for block in range(n_blocks):
        after = score(block + 1, qkv_b) if block + 1 < n_blocks else None
        mix(n_heads - 1, block, qkv_b, parts)
        parts = after

    for j, out in enumerate((c0, c1, c2, c3)):
        out[0] = ctx_buf[:, pl.ds(pl.multiple_of((me ^ j) * rows, rows), rows)].T


def whole(shape):
    return pl.BlockSpec(shape, lambda i, *_: (0,) * len(shape), pipeline_mode=pl.Buffered(1))


def attention(info, lens, sources, w_turned, bias, tables, caches, n_prompts, first):
    count, rows, width = sources[0].shape
    n_heads, span, _ = bias.shape
    head_dim = span // 3
    seq = rows * len(sources)
    prev = 0 if caches is None else 2
    hbm = pl.BlockSpec(memory_space=pl.ANY)
    source_spec = pl.BlockSpec((1, rows, width), lambda i, *_: (i, 0, 0))
    table = whole(tables[0].shape)
    cache_shape = jax.ShapeDtypeStruct((n_prompts, n_heads, head_dim, seq), jnp.bfloat16)
    cache_spec = pl.BlockSpec((1, n_heads, head_dim, seq), lambda i, *_: (i + first, 0, 0, 0))
    ctx_shape = jax.ShapeDtypeStruct((count, rows, n_heads * head_dim), jnp.bfloat16)
    ctx_spec = pl.BlockSpec((1, rows, n_heads * head_dim), lambda i, *_: (i, 0, 0))
    columns = pltpu.VMEM((span, seq), jnp.bfloat16)
    flops = count * seq * width * n_heads * 256 * 2 + count * n_heads * seq * seq * 256 * 2
    return pl.pallas_call(
        functools.partial(attn_kernel, n_heads, head_dim, rows, prev),
        grid_spec=pltpu.PrefetchScalarGridSpec(
            num_scalar_prefetch=2,
            grid=(count,),
            in_specs=[source_spec] * 4 + [whole(w_turned.shape), whole(bias.shape), table, table, table] + [hbm] * prev,
            out_specs=[cache_spec, cache_spec] + [ctx_spec] * 4,
            scratch_shapes=[columns, columns, pltpu.VMEM((seq, head_dim), jnp.bfloat16), pltpu.VMEM((n_heads * head_dim, seq), jnp.bfloat16)],
        ),
        out_shape=[cache_shape, cache_shape] + [ctx_shape] * 4,
        input_output_aliases={11: 0, 12: 1} if prev else {},
        compiler_params=pltpu.CompilerParams(dimension_semantics=("arbitrary",), vmem_limit_bytes=58 * 1024 * 1024),
        cost_estimate=pl.CostEstimate(flops=flops, bytes_accessed=count * seq * width * 4, transcendentals=count * n_heads * seq * seq // 2),
        name="qkv_attention",
    )(info, lens, *sources, w_turned, bias, *tables, *(caches or ()))


def out_kernel(n_shards, n_halves, n_quarters, n_prompts, shard_ref, x_ref, b_out_ref, b_down_ref, *rest):
    mlps, rest = rest[:n_quarters], rest[n_quarters:]
    contexts, weights, out_ref = rest[:n_halves * n_shards], rest[n_halves * n_shards:-1], rest[-1]
    step = pl.program_id(0)
    for q in range(n_quarters):
        half = q * n_halves // n_quarters

        @pl.when(step // (n_prompts // n_quarters) == q)
        def _(q=q, half=half):
            attn = b_out_ref[...]
            for c_ref, w_ref in zip(contexts[half * n_shards:(half + 1) * n_shards], weights):
                attn = attn + jnp.dot(c_ref[0], w_ref[...], preferred_element_type=jnp.float32)
            out_ref[0] = (x_ref[0].astype(jnp.float32) + attn + (mlps[q][0] + b_down_ref[...])).astype(jnp.bfloat16)


def finish(shard, hidden, mlps, b_out, b_down, contexts, w_out):
    n_shards, n_halves, n_quarters = len(contexts[0]), len(contexts), len(mlps)
    n_prompts, rows, width = hidden.shape
    span = contexts[0][0].shape[-1]
    block = pl.BlockSpec((1, rows, width), lambda i, *_: (i, 0, 0))
    w_specs = [
        pl.BlockSpec((span, width), lambda i, shard, j=j: (shard[0] ^ j, 0), pipeline_mode=pl.Buffered(1)) for j in range(n_shards)
    ]
    half, quarter = n_prompts // n_halves, n_prompts // n_quarters
    ctx_specs = [part_spec((rows, span), g * half, half) for g in range(n_halves) for _ in range(n_shards)]
    mlp_specs = [part_spec((rows, width), g * quarter, quarter) for g in range(n_quarters)]
    return pl.pallas_call(
        functools.partial(out_kernel, n_shards, n_halves, n_quarters, n_prompts),
        grid_spec=pltpu.PrefetchScalarGridSpec(
            num_scalar_prefetch=1,
            grid=(n_prompts,),
            in_specs=[block, whole((1, width)), whole((1, width))] + mlp_specs + ctx_specs + w_specs,
            out_specs=block,
        ),
        out_shape=jax.ShapeDtypeStruct(hidden.shape, jnp.bfloat16),
        compiler_params=pltpu.CompilerParams(dimension_semantics=("arbitrary",), vmem_limit_bytes=60 * 1024 * 1024),
        cost_estimate=pl.CostEstimate(flops=n_prompts * rows * width * width * 2, bytes_accessed=n_prompts * rows * width * 10, transcendentals=0),
        name="finish",
    )(shard, hidden, b_out, b_down, *mlps, *(c for group in contexts for c in group), *([w_out] * n_shards))


def solution(mesh):
    n_shards = mesh.shape['sp']
    row_spec = P('dp', 'sp', None)
    cache_spec = P('dp', 'sp', None, None)
    vec_spec = P(None)
    mat_spec = P(None, None)

    def swap(array, mask):
        return lax.ppermute(array, 'sp', [(i, i ^ mask) for i in range(n_shards)])

    def layer(hidden, seq_lens, ln1_gain, ln1_bias, ln2_gain, ln2_bias, w_qkv, b_qkv, w_out, b_out, w_up, b_up, w_down, b_down):
        n_prompts, rows, width = hidden.shape
        n_heads, _, head_dim = b_qkv.shape
        own_heads = n_heads // n_shards
        shard = lax.axis_index('sp')
        n_halves, n_quarters = 2, 4
        half = n_prompts // n_halves

        normed = norms(hidden, n_halves, n_quarters, ln1_gain[None], ln1_bias[None], ln2_gain[None], ln2_bias[None])
        attn_ins, mlp_ins = normed[:n_halves], list(normed[n_halves:])
        gathered = []
        for attn_in in attn_ins:
            near = swap(attn_in, 1)
            far = swap(attn_in, 2)
            relay = swap(far, 1)
            gathered.append((attn_in, near, far, relay))

        where = shard.astype(jnp.int32).reshape(1)
        w_turned = turned_columns(w_qkv, where, n_shards)
        b_heads = lax.dynamic_slice_in_dim(b_qkv, shard * own_heads, own_heads, axis=0).reshape(own_heads, 3 * head_dim, 1)
        tables = rotary_tables(rows * n_shards, head_dim)

        def mlp(m):
            count = m.shape[0]
            pre = jnp.dot(m.reshape(count * rows, width), w_up, preferred_element_type=jnp.float32) + b_up
            act = (0.5 * pre * (1.0 + lax.erf(pre * (0.5 ** 0.5)))).astype(jnp.bfloat16)
            return jnp.dot(act, w_down, preferred_element_type=jnp.float32).reshape(count, rows, width)

        mlps = [mlp(mlp_ins[q]) for q in range(n_quarters - 1)]
        caches, contexts = None, []
        for g, sources in enumerate(gathered):
            info = jnp.stack([shard, jnp.int32(g * half)]).astype(jnp.int32)
            k_cache, v_cache, *ctx = attention(info, seq_lens, sources, w_turned, b_heads, tables, caches, n_prompts, g * half)
            caches = (k_cache, v_cache)
            if g == 1:
                mlp_ins[-1], *ctx = lax.optimization_barrier((mlp_ins[-1], *ctx))
            swapped = [ctx[0]]
            for j in range(1, n_shards):
                swapped.append(swap(ctx[j], j))
            contexts.append(swapped)
        mlps.append(mlp(mlp_ins[-1]))
        out = finish(where, hidden, mlps, b_out[None], b_down[None], contexts, w_out)
        return out, jnp.swapaxes(caches[0], 2, 3), jnp.swapaxes(caches[1], 2, 3)

    return jax.shard_map(layer, mesh=mesh,
                         in_specs=(row_spec, P('dp'), vec_spec, vec_spec, vec_spec, vec_spec, mat_spec, P(None, None, None), mat_spec, vec_spec, mat_spec, vec_spec, mat_spec, vec_spec),
                         out_specs=(row_spec, cache_spec, cache_spec), check_vma=False)
```

```python
import functools

import jax
import jax.numpy as jnp
from jax import lax
from jax.experimental import pallas as pl
from jax.experimental.pallas import tpu as pltpu
from jax.sharding import PartitionSpec as P


LN_EPS = 1e-5
ROT_BASE = 10000.0
LOG2_E = 1.4426950408889634


def rotary_tables(n_positions, head_dim):
    rot_dim = head_dim // 4
    half_rot = rot_dim // 2
    inv_freq = ROT_BASE ** (-2.0 * jnp.arange(half_rot, dtype=jnp.float32) / rot_dim)
    angles = inv_freq[:, None] * jnp.arange(n_positions).astype(jnp.float32)[None, :]
    cosines, sines = jnp.cos(angles), jnp.sin(angles)
    rest = jnp.zeros((-rot_dim % 8, n_positions), jnp.float32)
    zeros = jnp.zeros_like(sines)
    keep = jnp.concatenate([cosines, cosines, rest + 1.0], axis=0)
    below = jnp.concatenate([-sines, zeros, rest], axis=0)
    above = jnp.concatenate([zeros, sines, rest], axis=0)
    return keep, below, above


def norm_kernel(n_halves, n_quarters, n_prompts, x_ref, g1_ref, b1_ref, g2_ref, b2_ref, *outs):
    step = pl.program_id(0)
    n_rows, piece = x_ref.shape[1], 16

    def run(a_part, m_part):
        for start in range(0, n_rows, piece):
            at = pl.ds(start, piece)
            rows = x_ref[0, at].astype(jnp.float32)
            centered = rows - jnp.mean(rows, axis=-1, keepdims=True)
            variance = jnp.mean(centered * centered, axis=-1, keepdims=True)
            normed = centered * lax.rsqrt(variance + LN_EPS)
            a_part[0, at] = (normed * g1_ref[...] + b1_ref[...]).astype(jnp.bfloat16)
            m_part[0, at] = (normed * g2_ref[...] + b2_ref[...]).astype(jnp.bfloat16)

    for q in range(n_quarters):
        @pl.when(step // (n_prompts // n_quarters) == q)
        def _(q=q):
            run(outs[q * n_halves // n_quarters], outs[n_halves + q])


def part_spec(shape, start, count):
    return pl.BlockSpec((1,) + shape, lambda i, *_: (jnp.clip(i - start, 0, count - 1), 0, 0))


def norms(hidden, n_halves, n_quarters, g1, b1, g2, b2):
    n_prompts, rows, width = hidden.shape
    vec = pl.BlockSpec((1, width), lambda i: (0, 0))
    parts = [(g * (n_prompts // n), n_prompts // n) for n in (n_halves, n_quarters) for g in range(n)]
    return pl.pallas_call(
        functools.partial(norm_kernel, n_halves, n_quarters, n_prompts),
        grid=(n_prompts,),
        in_specs=[pl.BlockSpec((1, rows, width), lambda i: (i, 0, 0)), vec, vec, vec, vec],
        out_specs=[part_spec((rows, width), *part) for part in parts],
        out_shape=[jax.ShapeDtypeStruct((count, rows, width), jnp.bfloat16) for _, count in parts],
        compiler_params=pltpu.CompilerParams(dimension_semantics=("arbitrary",)),
        cost_estimate=pl.CostEstimate(flops=n_prompts * rows * width * 200, bytes_accessed=n_prompts * rows * width * 6, transcendentals=0),
        name="norms",
    )(hidden, g1, b1, g2, b2)


def turn_kernel(shard_ref, w_ref, out_ref):
    out_ref[...] = w_ref[...].T


def turned_columns(w, shard, n_shards):
    depth, columns = w.shape
    span, piece = columns // n_shards, 256
    return pl.pallas_call(
        turn_kernel,
        grid_spec=pltpu.PrefetchScalarGridSpec(
            num_scalar_prefetch=1,
            grid=(depth // piece,),
            in_specs=[pl.BlockSpec((piece, span), lambda i, shard: (i, shard[0]))],
            out_specs=pl.BlockSpec((span, piece), lambda i, shard: (0, i)),
        ),
        out_shape=jax.ShapeDtypeStruct((span, depth), w.dtype),
        cost_estimate=pl.CostEstimate(flops=depth * span * 1000, bytes_accessed=depth * span * 4, transcendentals=0),
        name="turn",
    )(shard, w)


def attn_kernel(n_heads, head_dim, rows, prev, info_ref, len_ref, a0, a1, a2, a3, w_ref, bias_ref, keep_ref, below_ref, above_ref, *rest):
    k_out, v_out, c0, c1, c2, c3, qkv_a, qkv_b, k_turned, ctx_buf = rest[prev:]
    step = pl.program_id(0)
    me = info_ref[0]
    sources = (a0, a1, a2, a3)
    n_blocks = len(sources)
    scale = LOG2_E * head_dim ** -0.5
    half_rot = head_dim // 8
    turning = keep_ref.shape[0]
    span = 3 * head_dim

    length = len_ref[step + info_ref[1]]
    key = lax.broadcasted_iota(jnp.int32, (rows, rows), 0)
    causal = key <= lax.broadcasted_iota(jnp.int32, (rows, rows), 1)

    def project(head, j, qkv):
        at = pl.ds(pl.multiple_of((me ^ j) * rows, rows), rows)
        w_rows = w_ref[pl.ds(pl.multiple_of(head * span, span), span)]
        out = lax.dot_general(w_rows, sources[j][0], (((1,), (1,)), ((), ())), preferred_element_type=jnp.float32) + bias_ref[head]
        keep, below, above = keep_ref[:, at], below_ref[:, at], above_ref[:, at]

        def rotate(u):
            first = u[:turning]
            first = first * keep + pltpu.roll(first, turning - half_rot, 0) * below + pltpu.roll(first, half_rot, 0) * above
            return jnp.concatenate([first, u[turning:]], axis=0).astype(jnp.bfloat16)

        k_cols = rotate(out[head_dim:2 * head_dim])
        v_cols = out[2 * head_dim:].astype(jnp.bfloat16)
        qkv[:head_dim, at] = rotate(out[:head_dim])
        qkv[head_dim:2 * head_dim, at] = k_cols
        qkv[2 * head_dim:, at] = v_cols
        k_out[0, head, :, at] = k_cols
        v_out[0, head, :, at] = v_cols

    def turn(qkv):
        k_turned[...] = qkv[head_dim:2 * head_dim].T

    def score(block, qkv):
        q_cols = qkv[:head_dim, pl.ds(block * rows, rows)]
        parts = []
        for j in range(block + 1):
            s = jnp.dot(k_turned[pl.ds(j * rows, rows)], q_cols, preferred_element_type=jnp.float32)
            if j == block:
                s = jnp.where(causal, s, -jnp.inf)
            if (j + 1) * rows > n_blocks * rows // 2:
                s = jnp.where(key < length - j * rows, s, -jnp.inf)
            parts.append(s)
        return parts

    def mix(head, block, qkv, parts):
        at = pl.ds(block * rows, rows)
        top = functools.reduce(jnp.maximum, parts)
        top = jnp.max(top, axis=0, keepdims=True)
        parts = [jnp.exp2((s - top) * scale) for s in parts]
        total = jnp.sum(functools.reduce(jnp.add, parts), axis=0, keepdims=True)
        weights = jnp.concatenate([p.astype(jnp.bfloat16) for p in parts], axis=0)
        context = jnp.dot(qkv[2 * head_dim:, pl.ds(0, (block + 1) * rows)], weights, preferred_element_type=jnp.float32)
        ctx_buf[pl.ds(pl.multiple_of(head * head_dim, head_dim), head_dim), at] = (context / total).astype(jnp.bfloat16)

    def head_step(head, qkv, next_head, next_qkv):
        turn(qkv)
        parts = score(0, qkv)
        for block in range(n_blocks):
            after = score(block + 1, qkv) if block + 1 < n_blocks else None
            project(next_head, block, next_qkv)
            mix(head, block, qkv, parts)
            parts = after

    for j in range(n_blocks):
        project(0, j, qkv_a)

    def pair(t, carry):
        head_step(2 * t, qkv_a, 2 * t + 1, qkv_b)
        head_step(2 * t + 1, qkv_b, 2 * t + 2, qkv_a)
        return carry

    lax.fori_loop(0, n_heads // 2 - 1, pair, 0)
    head_step(n_heads - 2, qkv_a, n_heads - 1, qkv_b)
    turn(qkv_b)
    parts = score(0, qkv_b)
    for block in range(n_blocks):
        after = score(block + 1, qkv_b) if block + 1 < n_blocks else None
        mix(n_heads - 1, block, qkv_b, parts)
        parts = after

    for j, out in enumerate((c0, c1, c2, c3)):
        out[0] = ctx_buf[:, pl.ds(pl.multiple_of((me ^ j) * rows, rows), rows)].T


def whole(shape):
    return pl.BlockSpec(shape, lambda i, *_: (0,) * len(shape), pipeline_mode=pl.Buffered(1))


def attention(info, lens, sources, w_turned, bias, tables, caches, n_prompts, first):
    count, rows, width = sources[0].shape
    n_heads, span, _ = bias.shape
    head_dim = span // 3
    seq = rows * len(sources)
    prev = 0 if caches is None else 2
    hbm = pl.BlockSpec(memory_space=pl.ANY)
    source_spec = pl.BlockSpec((1, rows, width), lambda i, *_: (i, 0, 0))
    table = whole(tables[0].shape)
    cache_shape = jax.ShapeDtypeStruct((n_prompts, n_heads, head_dim, seq), jnp.bfloat16)
    cache_spec = pl.BlockSpec((1, n_heads, head_dim, seq), lambda i, *_: (i + first, 0, 0, 0))
    ctx_shape = jax.ShapeDtypeStruct((count, rows, n_heads * head_dim), jnp.bfloat16)
    ctx_spec = pl.BlockSpec((1, rows, n_heads * head_dim), lambda i, *_: (i, 0, 0))
    columns = pltpu.VMEM((span, seq), jnp.bfloat16)
    flops = count * seq * width * n_heads * 256 * 2 + count * n_heads * seq * seq * 256 * 2
    return pl.pallas_call(
        functools.partial(attn_kernel, n_heads, head_dim, rows, prev),
        grid_spec=pltpu.PrefetchScalarGridSpec(
            num_scalar_prefetch=2,
            grid=(count,),
            in_specs=[source_spec] * 4 + [whole(w_turned.shape), whole(bias.shape), table, table, table] + [hbm] * prev,
            out_specs=[cache_spec, cache_spec] + [ctx_spec] * 4,
            scratch_shapes=[columns, columns, pltpu.VMEM((seq, head_dim), jnp.bfloat16), pltpu.VMEM((n_heads * head_dim, seq), jnp.bfloat16)],
        ),
        out_shape=[cache_shape, cache_shape] + [ctx_shape] * 4,
        input_output_aliases={11: 0, 12: 1} if prev else {},
        compiler_params=pltpu.CompilerParams(dimension_semantics=("arbitrary",), vmem_limit_bytes=58 * 1024 * 1024),
        cost_estimate=pl.CostEstimate(flops=flops, bytes_accessed=count * seq * width * 4, transcendentals=count * n_heads * seq * seq // 2),
        name="qkv_attention",
    )(info, lens, *sources, w_turned, bias, *tables, *(caches or ()))


def out_kernel(n_shards, n_halves, n_quarters, n_prompts, shard_ref, x_ref, b_out_ref, b_down_ref, *rest):
    mlps, rest = rest[:n_quarters], rest[n_quarters:]
    contexts, (w_ref, out_ref, ctx_buf) = rest[:n_halves * n_shards], rest[n_halves * n_shards:]
    step, me = pl.program_id(0), shard_ref[0]
    for q in range(n_quarters):
        half = q * n_halves // n_quarters

        @pl.when(step // (n_prompts // n_quarters) == q)
        def _(q=q, half=half):
            for j, c_ref in enumerate(contexts[half * n_shards:(half + 1) * n_shards]):
                span = c_ref.shape[-1]
                ctx_buf[:, pl.ds(pl.multiple_of((me ^ j) * span, span), span)] = c_ref[0]
            attn = jnp.dot(ctx_buf[...], w_ref[...], preferred_element_type=jnp.float32) + b_out_ref[...]
            out_ref[0] = (x_ref[0].astype(jnp.float32) + attn + (mlps[q][0] + b_down_ref[...])).astype(jnp.bfloat16)


def finish(shard, hidden, mlps, b_out, b_down, contexts, w_out):
    n_shards, n_halves, n_quarters = len(contexts[0]), len(contexts), len(mlps)
    n_prompts, rows, width = hidden.shape
    span = contexts[0][0].shape[-1]
    block = pl.BlockSpec((1, rows, width), lambda i, *_: (i, 0, 0))
    half, quarter = n_prompts // n_halves, n_prompts // n_quarters
    ctx_specs = [part_spec((rows, span), g * half, half) for g in range(n_halves) for _ in range(n_shards)]
    mlp_specs = [part_spec((rows, width), g * quarter, quarter) for g in range(n_quarters)]
    return pl.pallas_call(
        functools.partial(out_kernel, n_shards, n_halves, n_quarters, n_prompts),
        grid_spec=pltpu.PrefetchScalarGridSpec(
            num_scalar_prefetch=1,
            grid=(n_prompts,),
            in_specs=[block, whole((1, width)), whole((1, width))] + mlp_specs + ctx_specs + [whole(w_out.shape)],
            out_specs=block,
            scratch_shapes=[pltpu.VMEM((rows, width), jnp.bfloat16)],
        ),
        out_shape=jax.ShapeDtypeStruct(hidden.shape, jnp.bfloat16),
        compiler_params=pltpu.CompilerParams(dimension_semantics=("arbitrary",), vmem_limit_bytes=60 * 1024 * 1024),
        cost_estimate=pl.CostEstimate(flops=n_prompts * rows * width * width * 2, bytes_accessed=n_prompts * rows * width * 10, transcendentals=0),
        name="finish",
    )(shard, hidden, b_out, b_down, *mlps, *(c for group in contexts for c in group), w_out)


def solution(mesh):
    n_shards = mesh.shape['sp']
    row_spec = P('dp', 'sp', None)
    cache_spec = P('dp', 'sp', None, None)
    vec_spec = P(None)
    mat_spec = P(None, None)

    def swap(array, mask):
        return lax.ppermute(array, 'sp', [(i, i ^ mask) for i in range(n_shards)])

    def layer(hidden, seq_lens, ln1_gain, ln1_bias, ln2_gain, ln2_bias, w_qkv, b_qkv, w_out, b_out, w_up, b_up, w_down, b_down):
        n_prompts, rows, width = hidden.shape
        n_heads, _, head_dim = b_qkv.shape
        own_heads = n_heads // n_shards
        shard = lax.axis_index('sp')
        n_halves, n_quarters = 2, 4
        half = n_prompts // n_halves

        normed = norms(hidden, n_halves, n_quarters, ln1_gain[None], ln1_bias[None], ln2_gain[None], ln2_bias[None])
        attn_ins, mlp_ins = normed[:n_halves], list(normed[n_halves:])
        gathered = []
        for attn_in in attn_ins:
            near = swap(attn_in, 1)
            far = swap(attn_in, 2)
            relay = swap(far, 1)
            gathered.append((attn_in, near, far, relay))

        where = shard.astype(jnp.int32).reshape(1)
        w_turned = turned_columns(w_qkv, where, n_shards)
        b_heads = lax.dynamic_slice_in_dim(b_qkv, shard * own_heads, own_heads, axis=0).reshape(own_heads, 3 * head_dim, 1)
        tables = rotary_tables(rows * n_shards, head_dim)

        def up(q):
            pre = jnp.dot(mlp_ins[q].reshape(-1, width), w_up, preferred_element_type=jnp.float32) + b_up
            return (0.5 * pre * (1.0 + lax.erf(pre * (0.5 ** 0.5)))).astype(jnp.bfloat16)

        def down(act):
            return jnp.dot(act, w_down, preferred_element_type=jnp.float32).reshape(-1, rows, width)

        acts = [up(q) for q in range(n_quarters - 1)]
        where_first, acts[-1] = lax.optimization_barrier((where, acts[-1]))
        mlps = [down(act) for act in acts]
        caches, contexts = None, []
        for g, sources in enumerate(gathered):
            info = jnp.concatenate([where_first if g == 0 else where, jnp.full(1, g * half, jnp.int32)])
            k_cache, v_cache, *ctx = attention(info, seq_lens, sources, w_turned, b_heads, tables, caches, n_prompts, g * half)
            caches = (k_cache, v_cache)
            if g == 1:
                mlp_ins[-1], *ctx = lax.optimization_barrier((mlp_ins[-1], *ctx))
            swapped = [ctx[0]]
            for j in range(1, n_shards):
                swapped.append(swap(ctx[j], j))
            contexts.append(swapped)
        mlps.append(down(up(n_quarters - 1)))
        out = finish(where, hidden, mlps, b_out[None], b_down[None], contexts, w_out)
        return out, jnp.swapaxes(caches[0], 2, 3), jnp.swapaxes(caches[1], 2, 3)

    return jax.shard_map(layer, mesh=mesh,
                         in_specs=(row_spec, P('dp'), vec_spec, vec_spec, vec_spec, vec_spec, mat_spec, P(None, None, None), mat_spec, vec_spec, mat_spec, vec_spec, mat_spec, vec_spec),
                         out_specs=(row_spec, cache_spec, cache_spec), check_vma=False)
```
